16 devices in a mesh: stage: 2 (over z), expert: 8 (over y, x, core).
Axes of the slice: x: 2, y: 2, z: 2, core: 2. Of those that a mesh axis runs over, the one named last changes fastest.
Arguments:
- x_act: bfloat16 [2, 8192, 2048], P('stage', 'expert')
- route_idx: int32 [2, 8192, 2], P('stage', 'expert')
- route_gate: float32 [2, 8192, 2], P('stage', 'expert')
- w_up: bfloat16 [2, 16, 2048, 1024], P('stage', 'expert')
- w_lin: bfloat16 [2, 16, 2048, 1024], P('stage', 'expert')
- w_down: bfloat16 [2, 16, 1024, 2048], P('stage', 'expert')
- dy_out: bfloat16 [2, 8192, 2048], P('stage', 'expert')
Outputs:
- output 1: bfloat16 [2, 8192, 2048], P('stage', 'expert')
- output 2: bfloat16 [2, 8192, 2048], P('stage', 'expert')
- output 3: bfloat16 [2, 16, 2048, 1024], P('stage', 'expert')
- output 4: bfloat16 [2, 16, 2048, 1024], P('stage', 'expert')
- output 5: bfloat16 [2, 16, 1024, 2048], P('stage', 'expert')
All inputs are finite; a program needn't handle non-finite values.
Results may differ from the reference program's by a relative error of at most 0.00121.
Values are sent between devices in bfloat16 or wider.
A program may use at most 1 GiB of HBM per device.

```python
import jax
import jax.numpy as jnp
from jax import lax

STAGE_DEVS = 2
EXPERT_DEVS = 8
TOKENS = 1024
D_MODEL = 2048
D_FF = 1024
EXPERTS = 16
TOP_K = 2

CAPACITY = 4 * TOKENS // EXPERTS
ROWS = EXPERT_DEVS * TOKENS


def draw_routing(rng_key):
    key_hot, key_bias, key_cell, key_perm, key_swap = jax.random.split(rng_key, 5)
    num_cells = EXPERTS * CAPACITY
    cell_ids = jnp.arange(num_cells, dtype=jnp.int32)
    cell_expert = cell_ids // CAPACITY
    cell_slot = cell_ids % CAPACITY
    hot_expert = jax.random.randint(key_hot, (), 0, EXPERTS)
    expert_bias = jax.random.randint(key_bias, (EXPERTS,), 0, 4) * 256
    cell_score = jax.random.randint(key_cell, (num_cells,), 0, 1024) + expert_bias[cell_expert]
    needed = (cell_slot == 0) | (cell_expert == hot_expert)
    cell_score = jnp.where(needed, 4096, cell_score)
    top_vals, chosen = lax.top_k(cell_score * num_cells + cell_ids, 2 * TOKENS)
    chosen_expert = jnp.sort(chosen) // CAPACITY
    expert_pairs = jnp.stack([chosen_expert[:TOKENS], chosen_expert[TOKENS:]], axis=1)
    expert_pairs = expert_pairs[jax.random.permutation(key_perm, TOKENS)]
    swap_flag = jax.random.randint(key_swap, (TOKENS, 1), 0, 2)
    return jnp.where(swap_flag == 1, expert_pairs[:, ::-1], expert_pairs).astype(jnp.int32)


def setup_inputs(seed: int = 0) -> dict:
    root_key = jax.random.key(seed)
    key_x, key_route, key_gate, key_up, key_lin, key_down, key_dy = jax.random.split(root_key, 7)
    shape_tok = (STAGE_DEVS, ROWS, D_MODEL)
    x_act = jax.random.normal(key_x, shape_tok, jnp.float32).astype(jnp.bfloat16)
    route_keys = jax.random.split(key_route, STAGE_DEVS * EXPERT_DEVS)
    route_idx = jax.vmap(draw_routing)(route_keys).reshape(STAGE_DEVS, ROWS, TOP_K)
    first_gate = jax.random.uniform(key_gate, (STAGE_DEVS, ROWS, 1), jnp.float32, 0.3, 0.7)
    route_gate = jnp.concatenate([first_gate, 1.0 - first_gate], axis=-1)
    shape_in = (STAGE_DEVS, EXPERTS, D_MODEL, D_FF)
    shape_out = (STAGE_DEVS, EXPERTS, D_FF, D_MODEL)
    w_up = (jax.random.normal(key_up, shape_in, jnp.float32) * D_MODEL ** -0.5).astype(jnp.bfloat16)
    w_lin = (jax.random.normal(key_lin, shape_in, jnp.float32) * D_MODEL ** -0.5).astype(jnp.bfloat16)
    w_down = (jax.random.normal(key_down, shape_out, jnp.float32) * D_FF ** -0.5).astype(jnp.bfloat16)
    dy_out = jax.random.normal(key_dy, shape_tok, jnp.float32).astype(jnp.bfloat16)
    return {"x_act": x_act, "route_idx": route_idx, "route_gate": route_gate, "w_up": w_up, "w_lin": w_lin, "w_down": w_down, "dy_out": dy_out}


def expert_block(x_src, idx_src, gate_src, dy_dst, w_up, w_lin, w_down):
    member = jnp.sum(jax.nn.one_hot(idx_src, EXPERTS, dtype=jnp.int32), axis=1)
    earlier = jnp.cumsum(member, axis=0) - member
    slot_pos = jnp.take_along_axis(earlier, idx_src, axis=1)
    x_copies = jnp.broadcast_to(x_src.astype(jnp.float32)[:, None, :], (TOKENS, TOP_K, D_MODEL))
    empty_rows = jnp.zeros((EXPERTS, CAPACITY, D_MODEL), jnp.float32)
    x_rows = empty_rows.at[idx_src, slot_pos].set(x_copies)
    pre_up = jnp.einsum("ecd,edf->ecf", x_rows, w_up)
    pre_lin = jnp.einsum("ecd,edf->ecf", x_rows, w_lin)
    act_up = jax.nn.silu(pre_up)
    hidden = (act_up * pre_lin).astype(jnp.bfloat16).astype(jnp.float32)
    out_rows = jnp.einsum("ecf,efd->ecd", hidden, w_down).astype(jnp.bfloat16).astype(jnp.float32)
    out_copies = out_rows[idx_src, slot_pos]
    y_tok = jnp.sum(gate_src[:, :, None] * out_copies, axis=1).astype(jnp.bfloat16)
    d_copies = (gate_src[:, :, None] * dy_dst.astype(jnp.float32)[:, None, :]).astype(jnp.bfloat16).astype(jnp.float32)
    d_rows = empty_rows.at[idx_src, slot_pos].set(d_copies)
    d_hidden = jnp.einsum("ecd,efd->ecf", d_rows, w_down).astype(jnp.bfloat16).astype(jnp.float32)
    sigmoid_up = jax.nn.sigmoid(pre_up)
    d_up = (d_hidden * pre_lin * sigmoid_up * (1.0 + pre_up * (1.0 - sigmoid_up))).astype(jnp.bfloat16).astype(jnp.float32)
    d_lin = (d_hidden * act_up).astype(jnp.bfloat16).astype(jnp.float32)
    g_up = jnp.einsum("ecd,ecf->edf", x_rows, d_up)
    g_lin = jnp.einsum("ecd,ecf->edf", x_rows, d_lin)
    g_down = jnp.einsum("ecf,ecd->efd", hidden, d_rows)
    dx_rows = (jnp.einsum("ecf,edf->ecd", d_up, w_up) + jnp.einsum("ecf,edf->ecd", d_lin, w_lin)).astype(jnp.bfloat16).astype(jnp.float32)
    dx_tok = jnp.sum(dx_rows[idx_src, slot_pos], axis=1).astype(jnp.bfloat16)
    return y_tok, dx_tok, g_up, g_lin, g_down


def stage_block(stage_args):
    x_stage, idx_stage, gate_stage, dy_stage, w_up, w_lin, w_down = stage_args
    w_up32 = w_up.astype(jnp.float32)
    w_lin32 = w_lin.astype(jnp.float32)
    w_down32 = w_down.astype(jnp.float32)

    def device_step(grad_sums, dev_block):
        block_out = expert_block(dev_block[0], dev_block[1], dev_block[2], dev_block[3], w_up32, w_lin32, w_down32)
        new_sums = (grad_sums[0] + block_out[2], grad_sums[1] + block_out[3], grad_sums[2] + block_out[4])
        return new_sums, (block_out[0], block_out[1])

    zero_grads = (jnp.zeros((EXPERTS, D_MODEL, D_FF), jnp.float32), jnp.zeros((EXPERTS, D_MODEL, D_FF), jnp.float32), jnp.zeros((EXPERTS, D_FF, D_MODEL), jnp.float32))
    dev_blocks = (x_stage.reshape(EXPERT_DEVS, TOKENS, D_MODEL), idx_stage.reshape(EXPERT_DEVS, TOKENS, TOP_K), gate_stage.reshape(EXPERT_DEVS, TOKENS, TOP_K), dy_stage.reshape(EXPERT_DEVS, TOKENS, D_MODEL))
    grad_sums, tok_outs = lax.scan(device_step, zero_grads, dev_blocks)
    y_stage = tok_outs[0].reshape(ROWS, D_MODEL)
    dx_stage = tok_outs[1].reshape(ROWS, D_MODEL)
    return y_stage, dx_stage, grad_sums[0].astype(jnp.bfloat16), grad_sums[1].astype(jnp.bfloat16), grad_sums[2].astype(jnp.bfloat16)


def reference(x_act, route_idx, route_gate, w_up, w_lin, w_down, dy_out):
    x_from = jnp.roll(x_act, 1, axis=0)
    idx_from = jnp.roll(route_idx, 1, axis=0)
    gate_from = jnp.roll(route_gate, 1, axis=0)
    y_out, dx_next, dw_up, dw_lin, dw_down = lax.map(stage_block, (x_from, idx_from, gate_from, dy_out, w_up, w_lin, w_down))
    dx_act = jnp.roll(dx_next, -1, axis=0)
    return y_out, dx_act, dw_up, dw_lin, dw_down
```

```python
import functools

import jax
import jax.numpy as jnp
from jax import lax
from jax.experimental import pallas as pl
from jax.experimental.pallas import tpu as pltpu
from jax.sharding import PartitionSpec as P


BF = jnp.bfloat16
F32 = jnp.float32
LAST = (((1,), (1,)), ((), ()))
FIRST = (((0,), (0,)), ((), ()))


def mm(a, b):
    return jnp.dot(a, b, preferred_element_type=F32)


def mm_t(a, b):
    return lax.dot_general(a, b, LAST, preferred_element_type=F32)


def params(n):
    return pltpu.CompilerParams(dimension_semantics=("arbitrary",) * n, vmem_limit_bytes=58 * 1024 * 1024)


def cost(flops, nbytes):
    return pl.CostEstimate(flops=int(flops), bytes_accessed=int(nbytes), transcendentals=0)


def place_rows(slot_row, capacity):
    tokens = slot_row.shape[-1]
    return lax.broadcasted_iota(jnp.int32, (capacity, tokens), 0) == slot_row


def pack_dh_body(cap, slot, gate, d0, d1, w, u, dh, place, scale, acc):
    k = pl.program_id(1)

    @pl.when(k == 0)
    def _():
        for blk in range(2):
            hit = place_rows(slot[0, blk : blk + 1, :], cap)
            place[blk] = jnp.where(hit, 1.0, 0.0).astype(BF)
            g = jnp.sum(jnp.where(hit, gate[0, blk : blk + 1, :], 0.0), axis=1, keepdims=True)
            scale[blk * cap : (blk + 1) * cap, :] = jnp.broadcast_to(g, (cap, 128))

    for blk, d in enumerate((d0, d1)):
        rows = slice(blk * cap, (blk + 1) * cap)
        u[0, rows, :] = (mm(place[blk], d[...]) * scale[rows, :1]).astype(BF)
    ff = acc.shape[1]
    for n in range(0, ff, 256):
        part = mm_t(u[0], w[0, n : n + 256, :])

        @pl.when(k == 0)
        def _():
            acc[:, n : n + 256] = part

        @pl.when(k > 0)
        def _():
            acc[:, n : n + 256] += part

    @pl.when(k == pl.num_programs(1) - 1)
    def _():
        dh[0] = acc[...].astype(BF)


def pack_dh(slot, gate, d0, d1, w_down, cap):
    experts, ff, width = w_down.shape
    tokens = d0.shape[0]
    kt = 512
    return pl.pallas_call(
        functools.partial(pack_dh_body, cap),
        name="pack_dh",
        grid=(experts, width // kt),
        in_specs=[
            pl.BlockSpec((1, 2, tokens), lambda e, k: (e, 0, 0)),
            pl.BlockSpec((1, 2, tokens), lambda e, k: (e, 0, 0)),
            pl.BlockSpec((tokens, kt), lambda e, k: (0, k)),
            pl.BlockSpec((tokens, kt), lambda e, k: (0, k)),
            pl.BlockSpec((1, ff, kt), lambda e, k: (e, 0, k)),
        ],
        out_specs=[
            pl.BlockSpec((1, 2 * cap, kt), lambda e, k: (e, 0, k)),
            pl.BlockSpec((1, 2 * cap, ff), lambda e, k: (e, 0, 0)),
        ],
        out_shape=[
            jax.ShapeDtypeStruct((experts, 2 * cap, width), BF),
            jax.ShapeDtypeStruct((experts, 2 * cap, ff), BF),
        ],
        scratch_shapes=[
            pltpu.VMEM((2, cap, tokens), BF),
            pltpu.VMEM((2 * cap, 128), F32),
            pltpu.VMEM((2 * cap, ff), F32),
        ],
        compiler_params=params(2),
        cost_estimate=cost(2 * experts * 2 * cap * width * (tokens + ff), 30e6),
    )(slot, gate, d0, d1, w_down)


def forward_body(cap, slot, x0, x1, wu, wl, dh, xr, hid, da, db, place, acc_a, acc_b):
    k = pl.program_id(1)

    @pl.when(k == 0)
    def _():
        for blk in range(2):
            hit = place_rows(slot[0, blk : blk + 1, :], cap)
            place[blk] = jnp.where(hit, 1.0, 0.0).astype(BF)

    for blk, x in enumerate((x0, x1)):
        xr[0, blk * cap : (blk + 1) * cap, :] = mm(place[blk], x[...]).astype(BF)
    ff = acc_a.shape[1]
    for acc, w in ((acc_a, wu), (acc_b, wl)):
        for n in range(0, ff, 256):
            part = mm(xr[0], w[0, :, n : n + 256])

            @pl.when(k == 0)
            def _():
                acc[:, n : n + 256] = part

            @pl.when(k > 0)
            def _():
                acc[:, n : n + 256] += part

    @pl.when(k == pl.num_programs(1) - 1)
    def _():
        step = 32

        @pl.loop(0, 2 * cap // step)
        def _(i):
            rows = pl.ds(pl.multiple_of(i * step, step), step)
            a = acc_a[rows, :]
            b = acc_b[rows, :]
            g = dh[0, rows, :].astype(F32)
            sig = jax.nn.sigmoid(a)
            act = a * sig
            hid[0, rows, :] = (act * b).astype(BF)
            da[0, rows, :] = (g * b * sig * (1.0 + a * (1.0 - sig))).astype(BF)
            db[0, rows, :] = (g * act).astype(BF)


def forward(slot, x0, x1, w_up, w_lin, dh, cap):
    experts, width, ff = w_up.shape
    tokens = x0.shape[0]
    kt = 512
    inner = pl.BlockSpec((1, 2 * cap, ff), lambda e, k: (e, 0, 0))
    return pl.pallas_call(
        functools.partial(forward_body, cap),
        name="expert_forward",
        grid=(experts, width // kt),
        in_specs=[
            pl.BlockSpec((1, 2, tokens), lambda e, k: (e, 0, 0)),
            pl.BlockSpec((tokens, kt), lambda e, k: (0, k)),
            pl.BlockSpec((tokens, kt), lambda e, k: (0, k)),
            pl.BlockSpec((1, kt, ff), lambda e, k: (e, k, 0)),
            pl.BlockSpec((1, kt, ff), lambda e, k: (e, k, 0)),
            inner,
        ],
        out_specs=[pl.BlockSpec((1, 2 * cap, kt), lambda e, k: (e, 0, k)), inner, inner, inner],
        out_shape=[jax.ShapeDtypeStruct((experts, 2 * cap, width), BF)]
        + [jax.ShapeDtypeStruct((experts, 2 * cap, ff), BF)] * 3,
        scratch_shapes=[
            pltpu.VMEM((2, cap, tokens), BF),
            pltpu.VMEM((2 * cap, ff), F32),
            pltpu.VMEM((2 * cap, ff), F32),
        ],
        compiler_params=params(2),
        cost_estimate=cost(2 * experts * 2 * cap * width * (tokens + 2 * ff), 40e6),
    )(slot, x0, x1, w_up, w_lin, dh)


def spread_init(cap, slot_col, spread):
    tokens = slot_col.shape[0]
    for blk in range(2):
        for e in range(2):
            col = slot_col[:, 2 * blk + e : 2 * blk + e + 1]
            hit = lax.broadcasted_iota(jnp.int32, (tokens, cap), 1) == col
            spread[blk, :, e * cap : (e + 1) * cap] = jnp.where(hit, 1.0, 0.0).astype(BF)


def dx_body(cap, slot_col, da, db, wu, wl, out0, out1, spread, rows):
    @pl.when(pl.program_id(0) == 0)
    def _():
        spread_init(cap, slot_col, spread)

    for e in range(2):
        dx = (mm_t(da[e], wu[e]) + mm_t(db[e], wl[e])).astype(BF)
        for blk in range(2):
            rows[blk, e * cap : (e + 1) * cap, :] = dx[blk * cap : (blk + 1) * cap, :]
    for blk, out in enumerate((out0, out1)):
        for t in range(0, out.shape[0], 256):
            out[t : t + 256, :] = mm(spread[blk, t : t + 256, :], rows[blk]).astype(BF)


def dx_dense(slot_col, da, db, w_up, w_lin, cap):
    experts, width, ff = w_up.shape
    tokens = slot_col.shape[0]
    nt = 512
    full = pl.BlockSpec((experts, 2 * cap, ff), lambda n: (0, 0, 0))
    wspec = pl.BlockSpec((experts, nt, ff), lambda n: (0, n, 0))
    out = pl.BlockSpec((tokens, nt), lambda n: (0, n))
    return pl.pallas_call(
        functools.partial(dx_body, cap),
        name="dx_dense",
        grid=(width // nt,),
        in_specs=[pl.BlockSpec((tokens, 4), lambda n: (0, 0)), full, full, wspec, wspec],
        out_specs=[out, out],
        out_shape=[jax.ShapeDtypeStruct((tokens, width), BF)] * 2,
        scratch_shapes=[
            pltpu.VMEM((2, tokens, experts * cap), BF),
            pltpu.VMEM((2, experts * cap, nt), BF),
        ],
        compiler_params=params(1),
        cost_estimate=cost(2 * experts * 2 * cap * width * (tokens + 2 * ff), 30e6),
    )(slot_col, da, db, w_up, w_lin)


def out_body(cap, slot_col, coef_col, hid, wd, out0, out1, spread, rows):
    @pl.when(pl.program_id(0) == 0)
    def _():
        spread_init(cap, slot_col, spread)

    for e in range(2):
        rows[e] = mm(hid[e], wd[e]).astype(BF)
    for blk, out in enumerate((out0, out1)):
        for t in range(0, out.shape[0], 256):
            parts = []
            for e in range(2):
                picked = mm(spread[blk, t : t + 256, e * cap : (e + 1) * cap], rows[e, blk * cap : (blk + 1) * cap, :])
                parts.append(picked * coef_col[t : t + 256, 2 * blk + e : 2 * blk + e + 1])
            out[t : t + 256, :] = (parts[0] + parts[1]).astype(BF)


def out_dense(slot_col, coef_col, hid, w_down, cap):
    experts, ff, width = w_down.shape
    tokens = slot_col.shape[0]
    nt = 512
    small = pl.BlockSpec((tokens, 4), lambda n: (0, 0))
    out = pl.BlockSpec((tokens, nt), lambda n: (0, n))
    return pl.pallas_call(
        functools.partial(out_body, cap),
        name="out_dense",
        grid=(width // nt,),
        in_specs=[
            small,
            small,
            pl.BlockSpec((experts, 2 * cap, ff), lambda n: (0, 0, 0)),
            pl.BlockSpec((experts, ff, nt), lambda n: (0, 0, n)),
        ],
        out_specs=[out, out],
        out_shape=[jax.ShapeDtypeStruct((tokens, width), BF)] * 2,
        scratch_shapes=[
            pltpu.VMEM((2, tokens, experts * cap), BF),
            pltpu.VMEM((experts, 2 * cap, nt), BF),
        ],
        compiler_params=params(1),
        cost_estimate=cost(2 * experts * 2 * cap * width * (tokens + ff), 25e6),
    )(slot_col, coef_col, hid, w_down)


def grad_in_body(groups, *refs):
    xr = refs[:groups]
    da = refs[groups : 2 * groups]
    db = refs[2 * groups : 3 * groups]
    gu, gl, turned = refs[3 * groups :]
    rows = xr[0].shape[1]
    for i in range(groups):
        turned[:, i * rows : (i + 1) * rows] = xr[i][0].T
    ff = gu.shape[2]
    for out, src in ((gu, da), (gl, db)):
        for n in range(0, ff, 256):
            acc = mm(turned[:, :rows], src[0][0, :, n : n + 256])
            for i in range(1, groups):
                acc += mm(turned[:, i * rows : (i + 1) * rows], src[i][0, :, n : n + 256])
            out[0, :, n : n + 256] = acc.astype(BF)


def grad_in(xr, da, db):
    groups = len(xr)
    experts, rows, width = xr[0].shape
    ff = da[0].shape[2]
    dt = 512
    inner = pl.BlockSpec((1, rows, ff), lambda e, d: (e, 0, 0))
    out = pl.BlockSpec((1, dt, ff), lambda e, d: (e, d, 0))
    return pl.pallas_call(
        functools.partial(grad_in_body, groups),
        name="grad_in",
        grid=(experts, width // dt),
        in_specs=[pl.BlockSpec((1, rows, dt), lambda e, d: (e, 0, d))] * groups + [inner] * (2 * groups),
        out_specs=[out, out],
        out_shape=[jax.ShapeDtypeStruct((experts, width, ff), BF)] * 2,
        scratch_shapes=[pltpu.VMEM((dt, groups * rows), BF)],
        compiler_params=params(2),
        cost_estimate=cost(4 * experts * groups * rows * width * ff, 50e6),
    )(*xr, *da, *db)


def grad_down_body(groups, *refs):
    hid = refs[:groups]
    u = refs[groups : 2 * groups]
    gd, turned = refs[2 * groups :]
    rows = hid[0].shape[1]

    @pl.when(pl.program_id(1) == 0)
    def _():
        for i in range(groups):
            turned[:, i * rows : (i + 1) * rows] = hid[i][0].T

    ff = gd.shape[1]
    for f in range(0, ff, 256):
        acc = mm(turned[f : f + 256, :rows], u[0][0])
        for i in range(1, groups):
            acc += mm(turned[f : f + 256, i * rows : (i + 1) * rows], u[i][0])
        gd[0, f : f + 256, :] = acc.astype(BF)


def grad_down(hid, u):
    groups = len(hid)
    experts, rows, ff = hid[0].shape
    width = u[0].shape[2]
    dt = 512
    return pl.pallas_call(
        functools.partial(grad_down_body, groups),
        name="grad_down",
        grid=(experts, width // dt),
        in_specs=[pl.BlockSpec((1, rows, ff), lambda e, d: (e, 0, 0))] * groups
        + [pl.BlockSpec((1, rows, dt), lambda e, d: (e, 0, d))] * groups,
        out_specs=pl.BlockSpec((1, ff, dt), lambda e, d: (e, 0, d)),
        out_shape=jax.ShapeDtypeStruct((experts, ff, width), BF),
        scratch_shapes=[pltpu.VMEM((ff, groups * rows), BF)],
        compiler_params=params(2),
        cost_estimate=cost(2 * experts * groups * rows * width * ff, 30e6),
    )(*hid, *u)


def solution(mesh):
    stages = mesh.shape["stage"]
    devs = mesh.shape["expert"]
    send_next = [(src, (src + 1) % stages) for src in range(stages)]
    send_back = [(src, (src - 1) % stages) for src in range(stages)]
    swap_core = [(i, i ^ 1) for i in range(devs)]
    first_hop = [(i, i ^ (4 if i & 1 else 2)) for i in range(devs)]
    second_hop = [(i, i ^ (2 if i & 1 else 4)) for i in range(devs)]
    tok_spec = P("stage", "expert", None)
    w_spec = P("stage", "expert", None, None)

    def hop(a, perm):
        return lax.ppermute(a, "expert", perm)

    def gather_blocks(block):
        r1 = hop(block, first_hop)
        r2 = hop(block, second_hop)
        r3 = hop(r1, second_hop)
        return [(b, hop(b, swap_core)) for b in (block, r1, r2, r3)]

    def device_step(x_act, route_idx, route_gate, w_up, w_lin, w_down, dy_out):
        tokens, width = x_act.shape[1:]
        experts = w_up.shape[1]
        capacity = 4 * tokens // (experts * devs)
        wu, wl, wd = w_up[0], w_lin[0], w_down[0]
        me = lax.axis_index("expert").astype(jnp.int32)
        core = me % 2
        m1 = jnp.where(core == 0, 2, 4)
        m2 = 6 - m1

        d_pairs = gather_blocks(dy_out[0])
        x_tok = lax.ppermute(x_act[0], "stage", send_next)
        x_pairs = gather_blocks(x_tok)

        meta = jnp.concatenate([route_idx[0].T.astype(F32), route_gate[0].T], axis=0)
        meta = lax.ppermute(meta, "stage", send_next)
        meta = lax.all_gather(meta, "expert", axis=0, tiled=False)
        order = jnp.stack([jnp.int32(0) * m1, 1 + 0 * m1, m1, m2 ^ 1, m2, m1 ^ 1, 6 + 0 * m1, 7 + 0 * m1])
        meta = jnp.take(meta, me ^ order, axis=0)
        ids = meta[:, :2].astype(jnp.int32)
        gates = meta[:, 2:]

        is_exp = ids[:, :, None, :] == (me * experts + jnp.arange(experts, dtype=jnp.int32))[None, None, :, None]
        member = jnp.any(is_exp, axis=1)
        tok = jnp.arange(tokens, dtype=jnp.int32)
        before = (tok[:, None] < tok[None, :]).astype(BF)
        earlier = jnp.einsum("bes,st->bet", member.astype(BF), before, preferred_element_type=F32).astype(jnp.int32)
        slot = jnp.where(member, earlier, -1)
        gate_exp = jnp.sum(jnp.where(is_exp, gates[:, :, None, :], 0.0), axis=1)

        def inside(block, units, unit_of):
            hit = functools.reduce(jnp.logical_or, [ids[block] // unit_of == u for u in units])
            return jnp.sum(hit.astype(jnp.int32), axis=0), jnp.sum(jnp.where(hit, gates[block], 0.0), axis=0)

        def coefs(children):
            total = sum(n for n, _ in children)
            return [jnp.where((n == 1) & (total == 2), g, 1.0)[:, None] for n, g in children]

        both = jnp.sum(member.astype(jnp.int32), axis=1) == 2
        local_coef = jnp.where(both[:, None, :], gate_exp, 1.0)

        slot_rows = [slot[2 * p : 2 * p + 2].transpose(1, 0, 2) for p in range(4)]
        gate_rows = [gate_exp[2 * p : 2 * p + 2].transpose(1, 0, 2) for p in range(4)]
        slot_cols = [slot[2 * p : 2 * p + 2].reshape(4, tokens).T for p in range(4)]
        coef_cols = [local_coef[2 * p : 2 * p + 2].reshape(4, tokens).T for p in range(4)]

        u, xr, hid, da, db = [], [], [], [], []
        for p in range(4):
            u_p, dh_p = pack_dh(slot_rows[p], gate_rows[p], *d_pairs[p], wd, capacity)
            xr_p, hid_p, da_p, db_p = forward(slot_rows[p], *x_pairs[p], wu, wl, dh_p, capacity)
            u.append(u_p)
            xr.append(xr_p)
            hid.append(hid_p)
            da.append(da_p)
            db.append(db_p)

        def add(parts):
            return functools.reduce(jnp.add, [a.astype(F32) for a in parts]).astype(BF)

        def weigh(parts, children):
            return functools.reduce(jnp.add, [a.astype(F32) * c for a, c in zip(parts, coefs(children))]).astype(BF)

        dx_part = []
        for p in range(4):
            mine, other = dx_dense(slot_cols[p], da[p], db[p], wu, wl, capacity)
            dx_part.append(add([mine, hop(other, swap_core)]))
        t2 = hop(dx_part[2], second_hop)
        t3 = hop(dx_part[3], second_hop)
        t1 = hop(add([dx_part[1], t3]), first_hop)
        dx_prev = lax.ppermute(add([dx_part[0], t1, t2]), "stage", send_back)

        per_chip = 2 * experts
        chip = me // 2
        y_part = []
        for p in range(4):
            mine, other = out_dense(slot_cols[p], coef_cols[p], hid[p], wd, capacity)
            kids = [inside(2 * p, [me], experts), inside(2 * p, [me ^ 1], experts)]
            y_part.append(weigh([mine, hop(other, swap_core)], kids))
        t2 = hop(y_part[2], second_hop)
        t3 = hop(y_part[3], second_hop)
        kids = [inside(2, [chip], per_chip), inside(2, [chip ^ (m2 // 2)], per_chip)]
        t1 = hop(weigh([y_part[1], t3], kids), first_hop)
        kids = [
            inside(0, [chip], per_chip),
            inside(0, [chip ^ (m1 // 2), chip ^ 3], per_chip),
            inside(0, [chip ^ (m2 // 2)], per_chip),
        ]
        y_tok = weigh([y_part[0], t1, t2], kids)

        g_up, g_lin = grad_in(xr, da, db)
        g_down = grad_down(hid, u)
        return y_tok[None], dx_prev[None], g_up[None], g_lin[None], g_down[None]

    return jax.shard_map(device_step, mesh=mesh, in_specs=(tok_spec, tok_spec, tok_spec, w_spec, w_spec, w_spec, tok_spec), out_specs=(tok_spec, tok_spec, w_spec, w_spec, w_spec), check_vma=False)
```
